32 devices in a mesh: seq: 8 (over z, y), head: 4 (over x, core).
Axes of the slice: x: 2, y: 2, z: 4, core: 2. Of those that a mesh axis runs over, the one named last changes fastest.
Arguments:
- tokens: bfloat16 [4096, 2048], P('seq'), may hold values from -100 to 100
- seq_ids: int32 [4096], P('seq'), may hold values from 0 to 15, never falling along the last dimension, each value on 1 to 1024 neighbouring positions
- w_query: bfloat16 [2048, 3072], P(None, 'head'), may hold values from -0.125 to 0.125
- w_down: bfloat16 [2048, 576], replicated, may hold values from -0.125 to 0.125
- latent_gain: float32 [512], replicated, may hold values from 0.1 to 1.9
- w_key_up: bfloat16 [16, 128, 512], P('head'), may hold values from -0.5 to 0.5
- w_value_up: bfloat16 [16, 512, 128], P('head'), may hold values from -0.25 to 0.25
- w_out: bfloat16 [2048, 2048], P('head'), may hold values from -0.125 to 0.125
Outputs:
- attended: bfloat16 [4096, 2048], P('seq', 'head')
The draws below stay inside these ranges and needn't reach their ends.
Inputs may be any that keep to these rules, and one draw needn't show every extreme that they name: `seq_ids`: prompt numbers never fall along the tokens; each of the 16 prompts holds 1 to 1024 tokens, one exactly 1024.
All inputs are finite; a program needn't handle non-finite values.
Results may differ from the reference program's by a relative error of at most 0.014.
Values may be sent and summed in bfloat16 or wider, within the bound.
A program may use at most 128 MiB of HBM per device.

```python
import math
import jax
import jax.numpy as jnp
import numpy as np
from jax import lax

D = 2048
HEADS = 16
NOPE = 128
ROPE = 64
LATENT = 512
VALUE = 128
NSEQ = 16
TOKENS = 4096
MOST = 1024


def draw_tokens(key, part):
    return jax.random.truncated_normal(key, -6.0, 6.0, (TOKENS, D), jnp.float32).astype(jnp.bfloat16)


def block_scale(own_key, extent, cuts, low, largest):
    level = 1.0
    for dim, blocks in cuts:
        draws = jax.random.uniform(jax.random.fold_in(jax.random.fold_in(own_key, 6), dim), (blocks,), jnp.float32, low / len(cuts), largest / len(cuts))
        level = level * jnp.repeat(jnp.exp(draws), extent[dim] // blocks).reshape((-1,) + (1,) * (len(extent) - 1 - dim))
    return level


def length_profile(amount, total, limit, slope):
    portions = [(1 << 20) // math.isqrt(rank ** slope) + 1 for rank in range(2, amount + 1)]
    spare, counts = total - limit - (amount - 1), [1] * (amount - 1)
    while spare > 0:
        candidates = [i for i in range(amount - 1) if counts[i] < limit]
        whole, budget = sum([portions[i] for i in candidates]), spare
        for i in candidates:
            addition = min(limit - counts[i], max(1, budget * portions[i] // whole), spare)
            counts[i] = counts[i] + addition
            spare = spare - addition
    return np.array([limit] + counts)


def ragged_sizes(rng, number_of, total, reach, slope):
    if number_of == 2:
        one = jax.random.randint(rng, (), max(1, total - reach), min(reach, total - 1) + 1)
        return jnp.stack([one, total - one])
    sizes = jnp.asarray(length_profile(number_of, total, reach, slope), jnp.int32)
    couples = (number_of - 1) // 2
    source_of, taker = sizes[1:1 + 2 * couples:2], sizes[2:2 + 2 * couples:2]
    room = jnp.minimum(source_of - 1, reach - taker)
    shifted = jax.random.randint(jax.random.fold_in(rng, 1), (couples,), 0, 1 << 20) % (room + 1)
    sizes = sizes.at[1:1 + 2 * couples:2].set(source_of - shifted).at[2:2 + 2 * couples:2].set(taker + shifted)
    return sizes[jax.random.permutation(jax.random.fold_in(rng, 2), number_of)]


def noise(stream_key, extent, scale, limit, cuts=(), kind=jnp.bfloat16):
    entries = jax.random.normal(stream_key, extent, jnp.float32) * scale
    if len(cuts) > 0:
        entries = block_scale(stream_key, extent, cuts, -0.22, 0.18) * entries
    return jnp.clip(entries, min=-limit, max=limit).astype(kind)


def setup_inputs(seed: int = 0) -> dict:
    streams_of = jax.random.split(jax.random.key(seed), 9)
    tokens = draw_tokens(jax.random.fold_in(streams_of[8], 71), 0)
    seq_ids = jnp.searchsorted(jnp.cumsum(ragged_sizes(streams_of[1], NSEQ, TOKENS, MOST, 2)), jnp.arange(TOKENS), side="right").astype(jnp.int32)
    w_query = noise(streams_of[2], (D, HEADS * (NOPE + ROPE)), D ** -0.5, 0.125, ((1, 4),))
    w_down = noise(streams_of[3], (D, LATENT + ROPE), D ** -0.5, 0.125)
    latent_gain = jnp.clip(1.0 + 0.18 * jax.random.normal(streams_of[4], (LATENT,), jnp.float32), 0.1, 1.9)
    w_key_up = noise(streams_of[5], (HEADS, NOPE, LATENT), NOPE ** -0.5, 0.5, ((0, 4),))
    w_value_up = noise(streams_of[6], (HEADS, LATENT, VALUE), LATENT ** -0.5, 0.25, ((0, 4),))
    w_out = noise(streams_of[7], (HEADS * VALUE, D), (HEADS * VALUE) ** -0.5, 0.125, ((0, 4),))
    return {"tokens": tokens, "seq_ids": seq_ids, "w_query": w_query, "w_down": w_down, "latent_gain": latent_gain, "w_key_up": w_key_up, "w_value_up": w_value_up, "w_out": w_out}


epsilon = 1e-06

def rotate(values, positions):
    half_width = values.shape[-1] // 2
    inverse = 10000.0 ** (-2.0 * jnp.arange(half_width, dtype=jnp.float32) / values.shape[-1])
    angles = positions.astype(jnp.float32)[:, None] * inverse[None, :]
    padding_dims = (1,) * (values.ndim - 2)
    cosine = jnp.cos(angles).reshape(angles.shape[:1] + padding_dims + angles.shape[1:])
    sine_table = jnp.sin(angles).reshape(angles.shape[:1] + padding_dims + angles.shape[1:])
    low_half = values[..., :half_width]
    high_half = values[..., half_width:]
    return jnp.concatenate([low_half * cosine - high_half * sine_table, high_half * cosine + low_half * sine_table], axis=-1)

def sequence_positions(seq_ids):
    row_index = jnp.arange(seq_ids.shape[0], dtype=jnp.int32)
    starts = jnp.concatenate([jnp.ones((1,), jnp.bool_), seq_ids[1:] != seq_ids[:-1]])
    seg_begin = lax.cummax(jnp.where(starts, row_index, 0), axis=0)
    return row_index - seg_begin

def reference(tokens, seq_ids, w_query, w_down, latent_gain, w_key_up, w_value_up, w_out):
    positions = sequence_positions(seq_ids)
    query = jnp.dot(tokens, w_query, preferred_element_type=jnp.float32).astype(jnp.bfloat16)
    query = query.reshape(TOKENS, HEADS, NOPE + ROPE)
    down = jnp.dot(tokens, w_down, preferred_element_type=jnp.float32)
    latent_raw = down[:, :LATENT]
    latent = (latent_raw * lax.rsqrt(lax.optimization_barrier(jnp.mean(latent_raw * latent_raw, axis=1, keepdims=True)) + epsilon) * latent_gain).astype(jnp.bfloat16)
    key_rope = rotate(down[:, LATENT:], positions).astype(jnp.bfloat16)
    query_rope = rotate(query[:, :, NOPE:].astype(jnp.float32), positions).astype(jnp.bfloat16)
    query_latent = jnp.einsum('thn,hnc->thc', query[:, :, :NOPE].astype(jnp.float32), w_key_up.astype(jnp.float32)).astype(jnp.bfloat16)
    query_full = jnp.concatenate([query_latent, query_rope], axis=2)
    key_full = jnp.concatenate([latent, key_rope], axis=1)
    score_scale = (NOPE + ROPE) ** (-0.5)
    query_block = min(512, TOKENS)
    window = min(MOST + query_block, TOKENS)

    def attend_block(query_first):
        query_part = lax.dynamic_slice_in_dim(query_full, query_first, query_block, 0)
        key_first = jnp.clip(query_first - MOST, 0, TOKENS - window).astype(jnp.int32)
        key_part = lax.dynamic_slice_in_dim(key_full, key_first, window, 0)
        query_segs = lax.dynamic_slice_in_dim(seq_ids, query_first, query_block, 0)
        key_segs = lax.dynamic_slice_in_dim(seq_ids, key_first, window, 0)
        query_index = query_first + jnp.arange(query_block, dtype=jnp.int32)
        key_index = key_first + jnp.arange(window, dtype=jnp.int32)
        scores = jnp.einsum('qhc,kc->hqk', query_part.astype(jnp.float32), key_part.astype(jnp.float32)) * score_scale
        allowed = (query_segs[:, None] == key_segs[None, :]) & (key_index[None, :] <= query_index[:, None])
        scores = jnp.where(allowed[None], scores, -jnp.inf)
        row_top = lax.optimization_barrier(jnp.max(scores, axis=2, keepdims=True))
        weights = jnp.where(allowed[None], jnp.exp(scores - row_top), 0.0)
        totals = lax.optimization_barrier(jnp.sum(weights, axis=2))
        mixed = jnp.einsum('hqk,kc->hqc', weights.astype(jnp.bfloat16).astype(jnp.float32), key_part[:, :LATENT].astype(jnp.float32))
        return (mixed / totals[:, :, None]).astype(jnp.bfloat16)
    firsts = jnp.arange(TOKENS // query_block, dtype=jnp.int32) * query_block
    latent_out = lax.map(attend_block, firsts)
    latent_out = latent_out.transpose(0, 2, 1, 3).reshape(TOKENS, HEADS, LATENT)
    head_out = jnp.einsum('thc,hcv->thv', latent_out.astype(jnp.float32), w_value_up.astype(jnp.float32)).astype(jnp.bfloat16)
    head_out = head_out.reshape(TOKENS, HEADS * VALUE)
    return jnp.dot(head_out, w_out, preferred_element_type=jnp.float32).astype(jnp.bfloat16)
```

```python
import functools
import math

import jax
import jax.numpy as jnp
from jax import lax
from jax.experimental import pallas as pl
from jax.experimental.pallas import tpu as pltpu
from jax.sharding import PartitionSpec as P

MESH = pl.DeviceIdType.MESH
epsilon = 1e-06
far_below = -1e30
PROMPTS = 16
f32 = jnp.float32
bf16 = jnp.bfloat16


def dot(a, b):
    return jnp.dot(a, b, preferred_element_type=f32)


def dot_t(a, b):
    return lax.dot_general(a, b, (((1,), (1,)), ((), ())), preferred_element_type=f32)


def attend_kernel(
    n, reach, tok_hbm, ids_ref, wq_hbm, wd_hbm, gain_ref, wk_hbm, wv_hbm, inv_ref, out_ref,
    tok, wq, wd, wk, wv, ids_r, lat, rop, q_s, k_s, v_s, beg, top, total, acc,
    load, s_id, r_id, s_key, r_key, s_fwd, r_fwd,
):
    rows = tok.shape[0]
    half = rows // 2
    latent_width = lat.shape[2]
    heads, _, value = acc.shape
    rope = inv_ref.shape[0] * 2
    nope = wk.shape[0] // heads
    seq = lax.axis_index("seq")
    head = lax.axis_index("head")
    parity = lax.rem(head, 2)
    mate = head + 1 - 2 * parity

    loads = [
        pltpu.make_async_copy(tok_hbm, tok, load.at[0]),
        pltpu.make_async_copy(wd_hbm, wd, load.at[1]),
        pltpu.make_async_copy(wq_hbm, wq, load.at[2]),
        pltpu.make_async_copy(wk_hbm, wk, load.at[3]),
    ]
    for h in range(heads):
        loads.append(
            pltpu.make_async_copy(
                wv_hbm.at[h], wv.at[:, h * value : (h + 1) * value], load.at[4 + h]
            )
        )
    for copy in loads:
        copy.start()

    barrier = pltpu.get_barrier_semaphore()
    pl.semaphore_signal(barrier, inc=1, device_id=(seq, mate), device_id_type=MESH)
    for d in range(1, reach + 1):

        @pl.when(seq + d < n)
        def _():
            pl.semaphore_signal(barrier, inc=1, device_id=(seq + d, head), device_id_type=MESH)

        @pl.when(seq >= d)
        def _():
            pl.semaphore_signal(barrier, inc=1, device_id=(seq - d, head), device_id_type=MESH)

    pl.semaphore_wait(
        barrier, 1 + jnp.minimum(seq, reach) + jnp.minimum(n - 1 - seq, reach)
    )

    def id_copy(d):
        return pltpu.make_async_remote_copy(
            src_ref=ids_ref, dst_ref=ids_r.at[d - 1], send_sem=s_id.at[d - 1],
            recv_sem=r_id.at[d - 1], device_id=(seq + d, head), device_id_type=MESH,
        )

    lat_rows = pl.ds(pl.multiple_of(parity * half, half), half)
    rop_rows = pl.ds(pl.multiple_of(parity * (half // 2), half // 2), half // 2)

    def key_copies(d):
        return [
            pltpu.make_async_remote_copy(
                src_ref=buf.at[0, part], dst_ref=buf.at[d, part], send_sem=s_key.at[d - 1, i],
                recv_sem=r_key.at[d - 1, i], device_id=(seq + d, head), device_id_type=MESH,
            )
            for i, (buf, part) in enumerate(((lat, lat_rows), (rop, rop_rows)))
        ]

    def forward_copies(d):
        return [
            pltpu.make_async_remote_copy(
                src_ref=buf.at[d, part], dst_ref=buf.at[d, part], send_sem=s_fwd.at[d - 1, i],
                recv_sem=r_fwd.at[d - 1, i], device_id=(seq, mate), device_id_type=MESH,
            )
            for i, (buf, part) in enumerate(((lat, lat_rows), (rop, rop_rows)))
        ]

    for d in range(1, reach + 1):

        @pl.when(seq + d < n)
        def _():
            id_copy(d).start()

        @pl.when(seq < d)
        def _():
            ids_r[d - 1] = jnp.full(ids_r.shape[1:], -1, jnp.int32)
            lat[d] = jnp.zeros(lat.shape[1:], bf16)
            rop[d] = jnp.zeros(rop.shape[1:], bf16)

    loads[0].wait()
    loads[1].wait()
    down = dot(tok[...], wd[...])
    raw = down[:, :latent_width]
    latent = (
        raw * lax.rsqrt(jnp.mean(raw * raw, axis=1, keepdims=True) + epsilon) * gain_ref[...]
    )
    lat[0] = latent.astype(bf16)

    for d in range(1, reach + 1):

        @pl.when(seq >= d)
        def _():
            id_copy(d).wait_recv()

    ids = ids_ref[...]
    marks = lax.broadcasted_iota(jnp.int32, (PROMPTS, rows), 0)
    below = jnp.sum((ids < marks).astype(f32), axis=1, keepdims=True)
    same = jnp.zeros((PROMPTS, 1), f32)
    for d in range(1, reach + 1):
        same = same + jnp.sum((ids_r[d - 1] == marks).astype(f32), axis=1, keepdims=True)
    begin = jnp.sum(jnp.where(ids == marks, below - same, 0.0), axis=0, keepdims=True)
    position = lax.broadcasted_iota(jnp.int32, (1, rows), 1).astype(f32) - begin
    angles = inv_ref[...] * position
    cosine, sine = jnp.cos(angles), jnp.sin(angles)
    cosine = jnp.concatenate([cosine] * (128 // (rope // 2)), axis=0).T[:, :rope]
    sine = jnp.concatenate([-sine, sine] * (128 // rope), axis=0).T[:, :rope]
    beg[...] = jnp.broadcast_to(begin, (128, rows)).T.astype(jnp.int32)

    def rotate(v):
        swapped = jnp.concatenate([v[:, rope // 2 :], v[:, : rope // 2]], axis=1)
        return (v * cosine + swapped * sine).astype(bf16)

    key_rope = rotate(down[:, latent_width:])
    rop[0] = jnp.concatenate([key_rope[:half], key_rope[half:]], axis=1)

    for d in range(1, reach + 1):

        @pl.when(seq + d < n)
        def _():
            for copy in key_copies(d):
                copy.start()

    loads[2].wait()
    query = dot(tok[...], wq[...]).astype(bf16)
    width = nope + rope
    pad = jnp.zeros((rows, q_s.shape[2] - width), bf16)
    for h in range(heads):
        at = h * width
        q_s[h] = jnp.concatenate(
            [
                query[:, at : at + nope],
                rotate(query[:, at + nope : at + width].astype(f32)),
                pad,
            ],
            axis=1,
        )
    for copy in loads[3:]:
        copy.wait()

    scale = (nope + rope) ** (-0.5) * math.log2(math.e)

    def expand(d):
        block = lat[d]
        keys = dot_t(block, wk[...]).astype(bf16)
        v_s[...] = dot(block, wv[...]).astype(bf16)
        packed = rop[d]
        tail = jnp.concatenate([packed[:, :rope], packed[:, rope:]], axis=0)
        tail = jnp.concatenate([tail, pad], axis=1)
        for h in range(heads):
            k_s[h] = jnp.concatenate([keys[:, h * nope : (h + 1) * nope], tail], axis=1)

    def piece(d, part, low, high):
        span = high - low
        q_at = part * half
        key_index = lax.broadcasted_iota(jnp.int32, (half, span), 1) + (low - d * rows)
        allowed = key_index >= beg[q_at : q_at + half, :1]
        if d == 0:
            allowed = allowed & (
                key_index <= lax.broadcasted_iota(jnp.int32, (half, span), 0) + q_at
            )
        for h in range(heads):
            mine = (h, slice(q_at, q_at + half))
            scores = dot_t(q_s[mine], k_s[h, low:high]) * scale
            scores = jnp.where(allowed, scores, far_below)
            best = jnp.max(scores, axis=1, keepdims=True)
            if d > 0:
                old = top[mine][:, :1]
                best = jnp.maximum(old, best)
                shrink = jnp.exp2(old - best)
            weights = jnp.exp2(scores - best)
            sums = jnp.sum(weights, axis=1, keepdims=True)
            mixed = dot(weights.astype(bf16), v_s[low:high, h * value : (h + 1) * value])
            if d > 0:
                sums = sums + total[mine][:, :1] * shrink
                mixed = mixed + acc[mine] * shrink
            if d < reach:
                top[mine] = jnp.broadcast_to(best, (half, 128))
                total[mine] = jnp.broadcast_to(sums, (half, 128))
                acc[mine] = mixed
            else:
                out_ref[q_at : q_at + half, h * value : (h + 1) * value] = (mixed / sums).astype(
                    bf16
                )

    expand(0)
    piece(0, 0, 0, half)
    piece(0, 1, 0, rows)
    for d in range(1, reach + 1):

        @pl.when(seq >= d)
        def _():
            for copy, forward in zip(key_copies(d), forward_copies(d)):
                copy.wait_recv()
                forward.start()

    for d in range(1, reach + 1):

        @pl.when(seq >= d)
        def _():
            for forward in forward_copies(d):
                forward.wait_recv()

        expand(d)
        piece(d, 0, 0, rows)
        piece(d, 1, half if d == reach else 0, rows)

    for d in range(1, reach + 1):

        @pl.when(seq + d < n)
        def _():
            id_copy(d).wait_send()
            for copy in key_copies(d):
                copy.wait_send()

        @pl.when(seq >= d)
        def _():
            for forward in forward_copies(d):
                forward.wait_send()


def scatter_kernel(
    chunks, ho_ref, w_hbm, out_ref, w, far_out, far_in, own_out, own_in, x_out, x_in,
    load, s_far, r_far, s_own, r_own, s_x, r_x,
):
    seq = lax.axis_index("seq")
    head = lax.axis_index("head")
    columns = out_ref.shape[1]
    depth = out_ref.shape[0] // chunks
    mate = head + 1 - 2 * lax.rem(head, 2)
    across = lax.rem(head + 2, 4)
    far = lax.rem(mate + 2, 4)
    loads = []
    for i, target in enumerate((far, across, mate, head)):
        part = pl.ds(pl.multiple_of(target * columns, columns), columns)
        loads.append(pltpu.make_async_copy(w_hbm.at[:, part], w.at[i], load.at[i]))
        loads[i].start()
    barrier = pltpu.get_barrier_semaphore()
    for other in (mate, across):
        pl.semaphore_signal(barrier, inc=1, device_id=(seq, other), device_id_type=MESH)
    pl.semaphore_wait(barrier, 2)

    def send(src, dst, c, s, r, other):
        return pltpu.make_async_remote_copy(
            src_ref=src.at[c], dst_ref=dst.at[c], send_sem=s.at[c], recv_sem=r.at[c],
            device_id=(seq, other), device_id_type=MESH,
        )

    def partial(c, i):
        return dot(ho_ref[c * depth : (c + 1) * depth], w[i])

    to_far = [send(far_out, far_in, c, s_far, r_far, mate) for c in range(chunks)]
    to_own = [send(own_out, own_in, c, s_own, r_own, mate) for c in range(chunks)]
    to_x = [send(x_out, x_in, c, s_x, r_x, across) for c in range(chunks)]
    loads[0].wait()
    for c in range(chunks):
        far_out[c] = partial(c, 0).astype(bf16)
        to_far[c].start()
    loads[1].wait()
    for c in range(chunks):
        mine = partial(c, 1)
        to_far[c].wait_recv()
        x_out[c] = (mine + far_in[c].astype(f32)).astype(bf16)
        to_x[c].start()
    loads[2].wait()
    for c in range(chunks):
        own_out[c] = partial(c, 2).astype(bf16)
        to_own[c].start()
    loads[3].wait()
    for c in range(chunks):
        mine = partial(c, 3)
        to_own[c].wait_recv()
        mine = mine + own_in[c].astype(f32)
        to_x[c].wait_recv()
        out_ref[c * depth : (c + 1) * depth] = (mine + x_in[c].astype(f32)).astype(bf16)
    for copy in to_far + to_own + to_x:
        copy.wait_send()


def local(tokens, seq_ids, w_query, w_down, latent_gain, w_key_up, w_value_up, w_out):
    rows, width = tokens.shape
    heads, nope, latent_width = w_key_up.shape
    value = w_value_up.shape[2]
    rope = w_down.shape[1] - latent_width
    n = lax.axis_size("seq")
    groups = lax.axis_size("head")
    reach = max(1, n // 4)
    padded = -(-(nope + rope) // 128) * 128
    inverse = 10000.0 ** (-2.0 * jnp.arange(rope // 2, dtype=f32) / rope)
    vmem = pl.BlockSpec(memory_space=pltpu.VMEM)
    anywhere = pl.BlockSpec(memory_space=pl.ANY)
    dma = pltpu.SemaphoreType.DMA
    head_out = pl.pallas_call(
        functools.partial(attend_kernel, n, reach),
        out_shape=jax.ShapeDtypeStruct((rows, heads * value), bf16),
        in_specs=[anywhere, vmem, anywhere, anywhere, vmem, anywhere, anywhere, vmem],
        out_specs=vmem,
        scratch_shapes=[
            pltpu.VMEM((rows, width), bf16),
            pltpu.VMEM(w_query.shape, bf16),
            pltpu.VMEM(w_down.shape, bf16),
            pltpu.VMEM((heads * nope, latent_width), bf16),
            pltpu.VMEM((latent_width, heads * value), bf16),
            pltpu.VMEM((reach, 1, rows), jnp.int32),
            pltpu.VMEM((reach + 1, rows, latent_width), bf16),
            pltpu.VMEM((reach + 1, rows // 2, 2 * rope), bf16),
            pltpu.VMEM((heads, rows, padded), bf16),
            pltpu.VMEM((heads, rows, padded), bf16),
            pltpu.VMEM((rows, heads * value), bf16),
            pltpu.VMEM((rows, 128), jnp.int32),
            pltpu.VMEM((heads, rows, 128), f32),
            pltpu.VMEM((heads, rows, 128), f32),
            pltpu.VMEM((heads, rows, value), f32),
            dma((4 + heads,)),
            dma((reach,)),
            dma((reach,)),
            dma((reach, 2)),
            dma((reach, 2)),
            dma((reach, 2)),
            dma((reach, 2)),
        ],
        compiler_params=pltpu.CompilerParams(
            collective_id=0, has_side_effects=True, vmem_limit_bytes=56 * 1024 * 1024
        ),
        name="attend",
    )(
        tokens,
        seq_ids.reshape(1, rows),
        w_query,
        w_down,
        latent_gain.reshape(1, latent_width),
        w_key_up.reshape(heads * nope, latent_width),
        w_value_up,
        inverse.reshape(rope // 2, 1),
    )
    columns = w_out.shape[1] // groups
    if groups != 4:
        partial = dot(head_out, w_out).astype(bf16)
        return lax.psum_scatter(partial, "head", scatter_dimension=1, tiled=True)
    chunks = 4
    block = (chunks, rows // chunks, columns)
    return pl.pallas_call(
        functools.partial(scatter_kernel, chunks),
        out_shape=jax.ShapeDtypeStruct((rows, columns), bf16),
        in_specs=[vmem, anywhere],
        out_specs=vmem,
        scratch_shapes=[pltpu.VMEM((4, w_out.shape[0], columns), bf16)]
        + [pltpu.VMEM(block, bf16)] * 6
        + [dma((4,))]
        + [dma((chunks,))] * 6,
        compiler_params=pltpu.CompilerParams(
            collective_id=1, has_side_effects=True, vmem_limit_bytes=32 * 1024 * 1024
        ),
        name="scatter",
    )(head_out, w_out)


def solution(mesh):
    return jax.shard_map(
        local,
        mesh=mesh,
        in_specs=(
            P("seq", None),
            P("seq"),
            P(None, "head"),
            P(),
            P(),
            P("head", None, None),
            P("head", None, None),
            P("head", None),
        ),
        out_specs=P("seq", "head"),
        check_vma=False,
    )
```

```python
import functools
import math

import jax
import jax.numpy as jnp
import numpy as np
from jax import lax
from jax.experimental import pallas as pl
from jax.experimental.pallas import tpu as pltpu
from jax.sharding import PartitionSpec as P

MESH = pl.DeviceIdType.MESH
epsilon = 1e-06
far_below = -1e30
PROMPTS = 16
f32 = jnp.float32
bf16 = jnp.bfloat16


def dot(a, b):
    return jnp.dot(a, b, preferred_element_type=f32)


def dot_t(a, b):
    return lax.dot_general(a, b, (((1,), (1,)), ((), ())), preferred_element_type=f32)


def attend_kernel(
    n, reach, chunks, tok_hbm, ids_ref, wq_hbm, wd_hbm, gain_ref, wk_hbm, wv_hbm, w_hbm, inv_ref,
    out_ref, tok, wq, wd, wk, wv, w, ids_r, pe, lat, rop, q_s, k_s, v_s, beg, top, total, acc, ho,
    far_out, far_in, own_out, own_in, x_out, x_in,
    load, s_id, r_id, s_key, r_key, s_fwd, r_fwd, s_far, r_far, s_own, r_own, s_x, r_x,
):
    rows = tok.shape[0]
    half = rows // 2
    latent_width = lat.shape[2]
    heads, _, value = acc.shape
    rope = inv_ref.shape[0] * 2
    nope = wk.shape[0] // heads
    seq = lax.axis_index("seq")
    head = lax.axis_index("head")
    parity = lax.rem(head, 2)
    mate = head + 1 - 2 * parity
    across = lax.rem(head + 2, 4)
    far = lax.rem(mate + 2, 4)
    columns = out_ref.shape[1]
    depth = rows // chunks

    loads = [
        pltpu.make_async_copy(tok_hbm, tok, load.at[0]),
        pltpu.make_async_copy(wd_hbm, wd, load.at[1]),
        pltpu.make_async_copy(wq_hbm, wq, load.at[2]),
        pltpu.make_async_copy(wk_hbm, wk, load.at[3]),
    ]
    for h in range(heads):
        loads.append(
            pltpu.make_async_copy(
                wv_hbm.at[h], wv.at[:, h * value : (h + 1) * value], load.at[4 + h]
            )
        )
    for i, target in enumerate((far, across, mate, head)):
        part = pl.ds(pl.multiple_of(target * columns, columns), columns)
        loads.append(pltpu.make_async_copy(w_hbm.at[:, part], w.at[i], load.at[4 + heads + i]))
    for copy in loads[:2]:
        copy.start()

    barrier = pltpu.get_barrier_semaphore()
    for other in (mate, across):
        pl.semaphore_signal(barrier, inc=1, device_id=(seq, other), device_id_type=MESH)
    for d in range(1, reach + 1):

        @pl.when(seq + d < n)
        def _():
            pl.semaphore_signal(barrier, inc=1, device_id=(seq + d, head), device_id_type=MESH)

        @pl.when(seq >= d)
        def _():
            pl.semaphore_signal(barrier, inc=1, device_id=(seq - d, head), device_id_type=MESH)

    pl.semaphore_wait(
        barrier, 2 + jnp.minimum(seq, reach) + jnp.minimum(n - 1 - seq, reach)
    )

    def id_copy(d):
        return pltpu.make_async_remote_copy(
            src_ref=ids_ref, dst_ref=ids_r.at[d - 1], send_sem=s_id.at[d - 1],
            recv_sem=r_id.at[d - 1], device_id=(seq + d, head), device_id_type=MESH,
        )

    lat_rows = pl.ds(pl.multiple_of(parity * half, half), half)
    rop_rows = pl.ds(pl.multiple_of(parity * (half // 2), half // 2), half // 2)

    def key_copies(d):
        return [
            pltpu.make_async_remote_copy(
                src_ref=buf.at[0, part], dst_ref=buf.at[d, part], send_sem=s_key.at[d - 1, i],
                recv_sem=r_key.at[d - 1, i], device_id=(seq + d, head), device_id_type=MESH,
            )
            for i, (buf, part) in enumerate(((lat, lat_rows), (rop, rop_rows)))
        ]

    def forward_copies(d):
        return [
            pltpu.make_async_remote_copy(
                src_ref=buf.at[d, part], dst_ref=buf.at[d, part], send_sem=s_fwd.at[d - 1, i],
                recv_sem=r_fwd.at[d - 1, i], device_id=(seq, mate), device_id_type=MESH,
            )
            for i, (buf, part) in enumerate(((lat, lat_rows), (rop, rop_rows)))
        ]

    for d in range(1, reach + 1):

        @pl.when(seq + d < n)
        def _():
            id_copy(d).start()

        @pl.when(seq < d)
        def _():
            ids_r[d - 1] = jnp.full(ids_r.shape[1:], -1, jnp.int32)
            lat[d] = jnp.zeros(lat.shape[1:], bf16)
            rop[d] = jnp.zeros(rop.shape[1:], bf16)

    loads[0].wait()
    loads[1].wait()
    for copy in loads[2:]:
        copy.start()

    def project(part):
        down = dot_t(tok[part], wd[...])
        raw = down[:, :latent_width]
        latent = (
            raw * lax.rsqrt(jnp.mean(raw * raw, axis=1, keepdims=True) + epsilon) * gain_ref[...]
        )
        lat[0, part] = latent.astype(bf16)
        pe[part] = down[:, latent_width:]

    def send_keys(i):
        for d in range(1, reach + 1):

            @pl.when(seq + d < n)
            def _():
                key_copies(d)[i].start()

    project(lat_rows)
    send_keys(0)
    project(pl.ds(pl.multiple_of((1 - parity) * half, half), half))

    for d in range(1, reach + 1):

        @pl.when(seq >= d)
        def _():
            id_copy(d).wait_recv()

    ids = ids_ref[...]
    marks = lax.broadcasted_iota(jnp.int32, (PROMPTS, rows), 0)
    below = jnp.sum((ids < marks).astype(f32), axis=1, keepdims=True)
    same = jnp.zeros((PROMPTS, 1), f32)
    for d in range(1, reach + 1):
        same = same + jnp.sum((ids_r[d - 1] == marks).astype(f32), axis=1, keepdims=True)
    begin = jnp.sum(jnp.where(ids == marks, below - same, 0.0), axis=0, keepdims=True)
    position = lax.broadcasted_iota(jnp.int32, (1, rows), 1).astype(f32) - begin
    angles = inv_ref[...] * position
    cosine, sine = jnp.cos(angles), jnp.sin(angles)
    cosine = jnp.concatenate([cosine] * (128 // (rope // 2)), axis=0).T[:, :rope]
    sine = jnp.concatenate([-sine, sine] * (128 // rope), axis=0).T[:, :rope]
    beg[...] = jnp.broadcast_to(begin, (128, rows)).T.astype(jnp.int32)

    def rotate(v):
        swapped = jnp.concatenate([v[:, rope // 2 :], v[:, : rope // 2]], axis=1)
        return (v * cosine + swapped * sine).astype(bf16)

    key_rope = rotate(pe[...])
    rop[0] = jnp.concatenate([key_rope[:half], key_rope[half:]], axis=1)

    send_keys(1)

    loads[2].wait()
    query = dot(tok[...], wq[...]).astype(bf16)
    width = nope + rope
    pad = jnp.zeros((rows, q_s.shape[2] - width), bf16)
    for h in range(heads):
        at = h * width
        q_s[h] = jnp.concatenate(
            [
                query[:, at : at + nope],
                rotate(query[:, at + nope : at + width].astype(f32)),
                pad,
            ],
            axis=1,
        )
    for copy in loads[3:]:
        copy.wait()

    scale = (nope + rope) ** (-0.5) * math.log2(math.e)

    def expand(d):
        block = lat[d]
        keys = dot_t(block, wk[...]).astype(bf16)
        v_s[...] = dot(block, wv[...]).astype(bf16)
        packed = rop[d]
        tail = jnp.concatenate([packed[:, :rope], packed[:, rope:]], axis=0)
        tail = jnp.concatenate([tail, pad], axis=1)
        for h in range(heads):
            k_s[h] = jnp.concatenate([keys[:, h * nope : (h + 1) * nope], tail], axis=1)

    def piece(d, part, low, high):
        span = high - low
        q_at = part * half
        key_index = lax.broadcasted_iota(jnp.int32, (half, span), 1) + (low - d * rows)
        allowed = key_index >= beg[q_at : q_at + half, :1]
        if d == 0:
            allowed = allowed & (
                key_index <= lax.broadcasted_iota(jnp.int32, (half, span), 0) + q_at
            )
        for h in range(heads):
            mine = (h, slice(q_at, q_at + half))
            scores = dot_t(q_s[mine], k_s[h, low:high]) * scale
            scores = jnp.where(allowed, scores, far_below)
            best = jnp.max(scores, axis=1, keepdims=True)
            if d > 0:
                old = top[mine][:, :1]
                best = jnp.maximum(old, best)
                shrink = jnp.exp2(old - best)
            weights = jnp.exp2(scores - best)
            sums = jnp.sum(weights, axis=1, keepdims=True)
            mixed = dot(weights.astype(bf16), v_s[low:high, h * value : (h + 1) * value])
            if d > 0:
                sums = sums + total[mine][:, :1] * shrink
                mixed = mixed + acc[mine] * shrink
            if d < reach:
                top[mine] = jnp.broadcast_to(best, (half, 128))
                total[mine] = jnp.broadcast_to(sums, (half, 128))
                acc[mine] = mixed
            else:
                ho[q_at : q_at + half, h * value : (h + 1) * value] = (mixed / sums).astype(
                    bf16
                )

    def send(src, dst, c, s, r, other):
        return pltpu.make_async_remote_copy(
            src_ref=src.at[c], dst_ref=dst.at[c], send_sem=s.at[c], recv_sem=r.at[c],
            device_id=(seq, other), device_id_type=MESH,
        )

    to_far = [send(far_out, far_in, c, s_far, r_far, mate) for c in range(chunks)]
    to_own = [send(own_out, own_in, c, s_own, r_own, mate) for c in range(chunks)]
    to_x = [send(x_out, x_in, c, s_x, r_x, across) for c in range(chunks)]

    def partial(c, i):
        return dot(ho[c * depth : (c + 1) * depth], w[i])

    def reduce_far(part):
        mine = range(part * chunks // 2, (part + 1) * chunks // 2)
        for c in mine:
            far_out[c] = partial(c, 0).astype(bf16)
            to_far[c].start()
        for c in mine:
            ours = partial(c, 1)
            to_far[c].wait_recv()
            x_out[c] = (ours + far_in[c].astype(f32)).astype(bf16)
            to_x[c].start()

    expand(0)
    piece(0, 0, 0, half)
    piece(0, 1, 0, rows)
    for d in range(1, reach + 1):

        @pl.when(seq >= d)
        def _():
            for copy, forward in zip(key_copies(d), forward_copies(d)):
                copy.wait_recv()
                forward.start()

    for d in range(1, reach + 1):

        @pl.when(seq >= d)
        def _():
            for forward in forward_copies(d):
                forward.wait_recv()

        expand(d)
        piece(d, 0, 0, rows)
        if d == reach:
            reduce_far(0)
        piece(d, 1, half if d == reach else 0, rows)

    reduce_far(1)
    for c in range(chunks):
        own_out[c] = partial(c, 2).astype(bf16)
        to_own[c].start()
    for c in range(chunks):
        mine = partial(c, 3)
        to_own[c].wait_recv()
        mine = mine + own_in[c].astype(f32)
        to_x[c].wait_recv()
        out_ref[c * depth : (c + 1) * depth] = (mine + x_in[c].astype(f32)).astype(bf16)
    for copy in to_far + to_own + to_x:
        copy.wait_send()

    for d in range(1, reach + 1):

        @pl.when(seq + d < n)
        def _():
            id_copy(d).wait_send()
            for copy in key_copies(d):
                copy.wait_send()

        @pl.when(seq >= d)
        def _():
            for forward in forward_copies(d):
                forward.wait_send()


def local(tokens, seq_ids, w_query, w_down, latent_gain, w_key_up, w_value_up, w_out):
    rows, width = tokens.shape
    heads, nope, latent_width = w_key_up.shape
    value = w_value_up.shape[2]
    rope = w_down.shape[1] - latent_width
    n = lax.axis_size("seq")
    groups = lax.axis_size("head")
    reach = max(1, n // 4)
    chunks = 4
    columns = w_out.shape[1] // groups
    block = (chunks, rows // chunks, columns)
    padded = -(-(nope + rope) // 128) * 128
    inverse = np.float32(10000.0) ** (
        np.float32(-2.0) * np.arange(rope // 2, dtype=np.float32) / np.float32(rope)
    )
    vmem = pl.BlockSpec(memory_space=pltpu.VMEM)
    anywhere = pl.BlockSpec(memory_space=pl.ANY)
    dma = pltpu.SemaphoreType.DMA
    return pl.pallas_call(
        functools.partial(attend_kernel, n, reach, chunks),
        out_shape=jax.ShapeDtypeStruct((rows, columns), bf16),
        in_specs=[anywhere, vmem, anywhere, anywhere, vmem, anywhere, anywhere, anywhere, vmem],
        out_specs=vmem,
        scratch_shapes=[
            pltpu.VMEM((rows, width), bf16),
            pltpu.VMEM(w_query.shape, bf16),
            pltpu.VMEM(w_down.shape[::-1], bf16),
            pltpu.VMEM((heads * nope, latent_width), bf16),
            pltpu.VMEM((latent_width, heads * value), bf16),
            pltpu.VMEM((groups, w_out.shape[0], columns), bf16),
            pltpu.VMEM((reach, 1, rows), jnp.int32),
            pltpu.VMEM((rows, rope), f32),
            pltpu.VMEM((reach + 1, rows, latent_width), bf16),
            pltpu.VMEM((reach + 1, rows // 2, 2 * rope), bf16),
            pltpu.VMEM((heads, rows, padded), bf16),
            pltpu.VMEM((heads, rows, padded), bf16),
            pltpu.VMEM((rows, heads * value), bf16),
            pltpu.VMEM((rows, 128), jnp.int32),
            pltpu.VMEM((heads, rows, 128), f32),
            pltpu.VMEM((heads, rows, 128), f32),
            pltpu.VMEM((heads, rows, value), f32),
            pltpu.VMEM((rows, heads * value), bf16),
        ]
        + [pltpu.VMEM(block, bf16)] * 6
        + [
            dma((4 + heads + groups,)),
            dma((reach,)),
            dma((reach,)),
            dma((reach, 2)),
            dma((reach, 2)),
            dma((reach, 2)),
            dma((reach, 2)),
        ]
        + [dma((chunks,))] * 6,
        compiler_params=pltpu.CompilerParams(
            collective_id=0, has_side_effects=True, vmem_limit_bytes=56 * 1024 * 1024
        ),
        name="attend",
    )(
        tokens,
        seq_ids.reshape(1, rows),
        w_query,
        w_down.T,
        latent_gain.reshape(1, latent_width),
        w_key_up.reshape(heads * nope, latent_width),
        w_value_up,
        w_out,
        jnp.asarray(inverse.reshape(rope // 2, 1)),
    )


def solution(mesh):
    return jax.shard_map(
        local,
        mesh=mesh,
        in_specs=(
            P("seq", None),
            P("seq"),
            P(None, "head"),
            P(),
            P(),
            P("head", None, None),
            P("head", None, None),
            P("head", None),
        ),
        out_specs=P("seq", "head"),
        check_vma=False,
    )
```

```python
import functools
import math

import jax
import jax.numpy as jnp
import numpy as np
from jax import lax
from jax.experimental import pallas as pl
from jax.experimental.pallas import tpu as pltpu
from jax.sharding import PartitionSpec as P

MESH = pl.DeviceIdType.MESH
epsilon = 1e-06
far_below = -1e30
PROMPTS = 16
f32 = jnp.float32
bf16 = jnp.bfloat16


def dot(a, b):
    return jnp.dot(a, b, preferred_element_type=f32)


def dot_t(a, b):
    return lax.dot_general(a, b, (((1,), (1,)), ((), ())), preferred_element_type=f32)


def attend_kernel(
    n, reach, chunks, tok_hbm, ids_ref, wq_hbm, wd_hbm, gain_ref, wk_hbm, wv_hbm, w_hbm, inv_ref,
    out_ref, tok, wq, wd, wk, wv, w, ids_r, pe, lat, rop, q_s, k_s, v_s, beg, top, total, acc, ho,
    far_out, far_in, own_out, own_in, x_out, x_in,
    load, s_id, r_id, s_key, r_key, s_fwd, r_fwd, s_far, r_far, s_own, r_own, s_x, r_x,
):
    rows = tok.shape[0]
    half = rows // 2
    latent_width = lat.shape[2]
    heads, _, value = acc.shape
    rope = inv_ref.shape[0] * 2
    nope = wk.shape[0] // heads
    seq = lax.axis_index("seq")
    head = lax.axis_index("head")
    parity = lax.rem(head, 2)
    mate = head + 1 - 2 * parity
    across = lax.rem(head + 2, 4)
    far = lax.rem(mate + 2, 4)
    columns = out_ref.shape[1]
    depth = rows // chunks

    loads = [
        pltpu.make_async_copy(tok_hbm, tok, load.at[0]),
        pltpu.make_async_copy(wd_hbm, wd, load.at[1]),
        pltpu.make_async_copy(wq_hbm, wq, load.at[2]),
        pltpu.make_async_copy(wk_hbm, wk, load.at[3]),
    ]
    for h in range(heads):
        loads.append(
            pltpu.make_async_copy(
                wv_hbm.at[h], wv.at[:, h * value : (h + 1) * value], load.at[4 + h]
            )
        )
    for i, target in enumerate((far, across, mate, head)):
        part = pl.ds(pl.multiple_of(target * columns, columns), columns)
        loads.append(pltpu.make_async_copy(w_hbm.at[:, part], w.at[i], load.at[4 + heads + i]))
    for copy in loads[:2]:
        copy.start()

    barrier = pltpu.get_barrier_semaphore()
    for other in (mate, across):
        pl.semaphore_signal(barrier, inc=1, device_id=(seq, other), device_id_type=MESH)
    for d in range(1, reach + 1):

        @pl.when(seq + d < n)
        def _():
            pl.semaphore_signal(barrier, inc=1, device_id=(seq + d, head), device_id_type=MESH)

        @pl.when(seq >= d)
        def _():
            pl.semaphore_signal(barrier, inc=1, device_id=(seq - d, head), device_id_type=MESH)

    pl.semaphore_wait(
        barrier, 2 + jnp.minimum(seq, reach) + jnp.minimum(n - 1 - seq, reach)
    )

    def id_copy(d):
        return pltpu.make_async_remote_copy(
            src_ref=ids_ref, dst_ref=ids_r.at[d - 1], send_sem=s_id.at[d - 1],
            recv_sem=r_id.at[d - 1], device_id=(seq + d, head), device_id_type=MESH,
        )

    lat_rows = pl.ds(pl.multiple_of(parity * half, half), half)
    rop_rows = pl.ds(pl.multiple_of(parity * (half // 2), half // 2), half // 2)

    def key_copies(d):
        return [
            pltpu.make_async_remote_copy(
                src_ref=buf.at[0, part], dst_ref=buf.at[d, part], send_sem=s_key.at[d - 1, i],
                recv_sem=r_key.at[d - 1, i], device_id=(seq + d, head), device_id_type=MESH,
            )
            for i, (buf, part) in enumerate(((lat, lat_rows), (rop, rop_rows)))
        ]

    def forward_copies(d):
        return [
            pltpu.make_async_remote_copy(
                src_ref=buf.at[d, part], dst_ref=buf.at[d, part], send_sem=s_fwd.at[d - 1, i],
                recv_sem=r_fwd.at[d - 1, i], device_id=(seq, mate), device_id_type=MESH,
            )
            for i, (buf, part) in enumerate(((lat, lat_rows), (rop, rop_rows)))
        ]

    for d in range(1, reach + 1):

        @pl.when(seq + d < n)
        def _():
            id_copy(d).start()

        @pl.when(seq < d)
        def _():
            ids_r[d - 1] = jnp.full(ids_r.shape[1:], -1, jnp.int32)
            lat[d] = jnp.zeros(lat.shape[1:], bf16)
            rop[d] = jnp.zeros(rop.shape[1:], bf16)

    loads[0].wait()
    loads[1].wait()
    for copy in loads[2:]:
        copy.start()

    def project(part):
        down = dot_t(tok[part], wd[...])
        raw = down[:, :latent_width]
        latent = (
            raw * lax.rsqrt(jnp.mean(raw * raw, axis=1, keepdims=True) + epsilon) * gain_ref[...]
        )
        lat[0, part] = latent.astype(bf16)
        pe[part] = down[:, latent_width:]

    def send_keys(i):
        for d in range(1, reach + 1):

            @pl.when(seq + d < n)
            def _():
                key_copies(d)[i].start()

    project(lat_rows)
    send_keys(0)
    project(pl.ds(pl.multiple_of((1 - parity) * half, half), half))

    for d in range(1, reach + 1):

        @pl.when(seq >= d)
        def _():
            id_copy(d).wait_recv()

    ids = ids_ref[...]
    marks = lax.broadcasted_iota(jnp.int32, (PROMPTS, rows), 0)
    below = jnp.sum((ids < marks).astype(f32), axis=1, keepdims=True)
    same = jnp.zeros((PROMPTS, 1), f32)
    for d in range(1, reach + 1):
        same = same + jnp.sum((ids_r[d - 1] == marks).astype(f32), axis=1, keepdims=True)
    begin = jnp.sum(jnp.where(ids == marks, below - same, 0.0), axis=0, keepdims=True)
    position = lax.broadcasted_iota(jnp.int32, (1, rows), 1).astype(f32) - begin
    angles = inv_ref[...] * position
    cosine, sine = jnp.cos(angles), jnp.sin(angles)
    cosine = jnp.concatenate([cosine] * (128 // (rope // 2)), axis=0).T[:, :rope]
    sine = jnp.concatenate([-sine, sine] * (128 // rope), axis=0).T[:, :rope]
    beg[...] = jnp.broadcast_to(begin, (128, rows)).T.astype(jnp.int32)

    def rotate(v):
        swapped = jnp.concatenate([v[:, rope // 2 :], v[:, : rope // 2]], axis=1)
        return (v * cosine + swapped * sine).astype(bf16)

    key_rope = rotate(pe[...])
    rop[0] = jnp.concatenate([key_rope[:half], key_rope[half:]], axis=1)

    send_keys(1)

    loads[2].wait()
    query = dot(tok[...], wq[...]).astype(bf16)
    width = nope + rope
    pad = jnp.zeros((rows, q_s.shape[2] - width), bf16)
    for h in range(heads):
        at = h * width
        q_s[h] = jnp.concatenate(
            [
                query[:, at : at + nope],
                rotate(query[:, at + nope : at + width].astype(f32)),
                pad,
            ],
            axis=1,
        )
    for copy in loads[3:]:
        copy.wait()

    scale = (nope + rope) ** (-0.5) * math.log2(math.e)

    def expand(d):
        block = lat[d]
        keys = dot_t(block, wk[...]).astype(bf16)
        v_s[...] = dot(block, wv[...]).astype(bf16)
        packed = rop[d]
        tail = jnp.concatenate([packed[:, :rope], packed[:, rope:]], axis=0)
        tail = jnp.concatenate([tail, pad], axis=1)
        for h in range(heads):
            k_s[h] = jnp.concatenate([keys[:, h * nope : (h + 1) * nope], tail], axis=1)

    def piece(d, part, low, high):
        span = high - low
        q_at = part * half
        key_index = lax.broadcasted_iota(jnp.int32, (half, span), 1) + (low - d * rows)
        allowed = key_index >= beg[q_at : q_at + half, :1]
        if d == 0:
            allowed = allowed & (
                key_index <= lax.broadcasted_iota(jnp.int32, (half, span), 0) + q_at
            )
        for h in range(heads):
            mine = (h, slice(q_at, q_at + half))
            scores = dot_t(q_s[mine], k_s[h, low:high]) * scale
            scores = jnp.where(allowed, scores, far_below)
            best = jnp.max(scores, axis=1, keepdims=True)
            if d > 0:
                old = top[mine][:, :1]
                best = jnp.maximum(old, best)
                shrink = jnp.exp2(old - best)
            weights = jnp.exp2(scores - best)
            sums = jnp.sum(weights, axis=1, keepdims=True)
            mixed = dot(weights.astype(bf16), v_s[low:high, h * value : (h + 1) * value])
            if d > 0:
                sums = sums + total[mine][:, :1] * shrink
                mixed = mixed + acc[mine] * shrink
            if d < reach:
                top[mine] = jnp.broadcast_to(best, (half, 128))
                total[mine] = jnp.broadcast_to(sums, (half, 128))
                acc[mine] = mixed
            else:
                ho[q_at : q_at + half, h * value : (h + 1) * value] = (mixed / sums).astype(
                    bf16
                )

    def send(src, dst, c, s, r, other):
        return pltpu.make_async_remote_copy(
            src_ref=src.at[c], dst_ref=dst.at[c], send_sem=s.at[c], recv_sem=r.at[c],
            device_id=(seq, other), device_id_type=MESH,
        )

    to_far = [send(far_out, far_in, c, s_far, r_far, mate) for c in range(chunks)]
    to_own = [send(own_out, own_in, c, s_own, r_own, mate) for c in range(chunks)]
    to_x = [send(x_out, x_in, c, s_x, r_x, across) for c in range(chunks)]

    def partial(c, i):
        return dot(ho[c * depth : (c + 1) * depth], w[i])

    def reduce_far(part):
        mine = range(part * chunks // 2, (part + 1) * chunks // 2)
        for c in mine:
            far_out[c] = partial(c, 0).astype(bf16)
            to_far[c].start()
        for c in mine:
            ours = partial(c, 1)
            to_far[c].wait_recv()
            x_out[c] = (ours + far_in[c].astype(f32)).astype(bf16)
            to_x[c].start()

    def pass_on(d):
        @pl.when(seq >= d)
        def _():
            for copy, forward in zip(key_copies(d), forward_copies(d)):
                copy.wait_recv()
                forward.start()

    expand(0)
    piece(0, 0, 0, half)
    pass_on(1)
    piece(0, 1, 0, rows)
    for d in range(1, reach + 1):

        @pl.when(seq >= d)
        def _():
            for forward in forward_copies(d):
                forward.wait_recv()

        expand(d)
        piece(d, 0, 0, rows)
        if d == reach:
            reduce_far(0)
        else:
            pass_on(d + 1)
        piece(d, 1, half if d == reach else 0, rows)

    reduce_far(1)
    for c in range(chunks):
        own_out[c] = partial(c, 2).astype(bf16)
        to_own[c].start()
    for c in range(chunks):
        mine = partial(c, 3)
        to_own[c].wait_recv()
        mine = mine + own_in[c].astype(f32)
        to_x[c].wait_recv()
        out_ref[c * depth : (c + 1) * depth] = (mine + x_in[c].astype(f32)).astype(bf16)
    for copy in to_far + to_own + to_x:
        copy.wait_send()

    for d in range(1, reach + 1):

        @pl.when(seq + d < n)
        def _():
            id_copy(d).wait_send()
            for copy in key_copies(d):
                copy.wait_send()

        @pl.when(seq >= d)
        def _():
            for forward in forward_copies(d):
                forward.wait_send()


def local(tokens, seq_ids, w_query, w_down, latent_gain, w_key_up, w_value_up, w_out):
    rows, width = tokens.shape
    heads, nope, latent_width = w_key_up.shape
    value = w_value_up.shape[2]
    rope = w_down.shape[1] - latent_width
    n = lax.axis_size("seq")
    groups = lax.axis_size("head")
    reach = max(1, n // 4)
    chunks = 4
    columns = w_out.shape[1] // groups
    block = (chunks, rows // chunks, columns)
    padded = -(-(nope + rope) // 128) * 128
    inverse = np.float32(10000.0) ** (
        np.float32(-2.0) * np.arange(rope // 2, dtype=np.float32) / np.float32(rope)
    )
    vmem = pl.BlockSpec(memory_space=pltpu.VMEM)
    anywhere = pl.BlockSpec(memory_space=pl.ANY)
    dma = pltpu.SemaphoreType.DMA
    return pl.pallas_call(
        functools.partial(attend_kernel, n, reach, chunks),
        out_shape=jax.ShapeDtypeStruct((rows, columns), bf16),
        in_specs=[anywhere, vmem, anywhere, anywhere, vmem, anywhere, anywhere, anywhere, vmem],
        out_specs=vmem,
        scratch_shapes=[
            pltpu.VMEM((rows, width), bf16),
            pltpu.VMEM(w_query.shape, bf16),
            pltpu.VMEM(w_down.shape[::-1], bf16),
            pltpu.VMEM((heads * nope, latent_width), bf16),
            pltpu.VMEM((latent_width, heads * value), bf16),
            pltpu.VMEM((groups, w_out.shape[0], columns), bf16),
            pltpu.VMEM((reach, 1, rows), jnp.int32),
            pltpu.VMEM((rows, rope), f32),
            pltpu.VMEM((reach + 1, rows, latent_width), bf16),
            pltpu.VMEM((reach + 1, rows // 2, 2 * rope), bf16),
            pltpu.VMEM((heads, rows, padded), bf16),
            pltpu.VMEM((heads, rows, padded), bf16),
            pltpu.VMEM((rows, heads * value), bf16),
            pltpu.VMEM((rows, 128), jnp.int32),
            pltpu.VMEM((heads, rows, 128), f32),
            pltpu.VMEM((heads, rows, 128), f32),
            pltpu.VMEM((heads, rows, value), f32),
            pltpu.VMEM((rows, heads * value), bf16),
        ]
        + [pltpu.VMEM(block, bf16)] * 6
        + [
            dma((4 + heads + groups,)),
            dma((reach,)),
            dma((reach,)),
            dma((reach, 2)),
            dma((reach, 2)),
            dma((reach, 2)),
            dma((reach, 2)),
        ]
        + [dma((chunks,))] * 6,
        compiler_params=pltpu.CompilerParams(
            collective_id=0, has_side_effects=True, vmem_limit_bytes=56 * 1024 * 1024
        ),
        name="attend",
    )(
        tokens,
        seq_ids.reshape(1, rows),
        w_query,
        w_down.T,
        latent_gain.reshape(1, latent_width),
        w_key_up.reshape(heads * nope, latent_width),
        w_value_up,
        w_out,
        jnp.asarray(inverse.reshape(rope // 2, 1)),
    )


def solution(mesh):
    return jax.shard_map(
        local,
        mesh=mesh,
        in_specs=(
            P("seq", None),
            P("seq"),
            P(None, "head"),
            P(),
            P(),
            P("head", None, None),
            P("head", None, None),
            P("head", None),
        ),
        out_specs=P("seq", "head"),
        check_vma=False,
    )
```
